32 devices in a mesh: ka: 8 (over z, core), band: 4 (over y, x).
Axes of the slice: x: 2, y: 2, z: 4, core: 2. Of those that a mesh axis runs over, the one named last changes fastest.
Arguments:
- occ_rows: bfloat16 [8, 2048, 128], P('ka', 'band'), may hold values from -0.5 to 0.5
- vir_rows: bfloat16 [8, 2048, 896], P('ka', 'band'), may hold values from -0.1875 to 0.1875
- trial_vectors: float32 [8, 2, 128, 896], P('ka', None, None, 'band'), may hold values from -6 to 6
- occ_energy: float32 [8, 128], P('ka'), may hold values from -1.2 to -0.3
- vir_energy: float32 [8, 896], P('ka', 'band'), may hold values from 0.1 to 1.5
- coulomb: bfloat16 [2048, 2048], P('band'), may hold values from -0.09375 to 0.09375
- exch_kernel: bfloat16 [8, 2048, 2048], P(None, 'band'), as said below
- minus_table: int32 [8, 8], replicated, may hold values from 0 to 7, as said below
Outputs:
- sigma_vectors: float32 [8, 2, 128, 896], P('ka', None, None, 'band')
The draws below stay inside these ranges and needn't reach their ends.
Inputs may be any that keep to these rules, and one draw needn't show every extreme that they name: minus_table[k, q] is the k-point k - q on a group of 8 k-points: every row and every column holds each index once, and one q gives minus_table[k, q] == k for every k. Each exch_kernel[q] is symmetric.
All inputs are finite; a program needn't handle non-finite values.
Results may differ from the reference program's by a relative error of at most 0.0051.
Values may be sent and summed in bfloat16 or wider, within the bound.
No kernel may reach another device: no remote copies, remote signals or barrier semaphores. Data moves between devices by JAX's collectives and lax.ppermute only.
A program may use at most 128 MiB of HBM per device.

```python
import jax
import jax.numpy as jnp
from jax import lax

NOCC = 128
NVIR = 896
NAUX = 2048
NVEC = 2
NK = 8


def draw_minus_table(key, part):
    labels = jax.random.permutation(jax.random.fold_in(key, 11), NK).astype(jnp.int32)
    difference = (labels[:, None] - labels[None, :]) % NK
    inverse = jnp.argsort(labels).astype(jnp.int32)
    return inverse[difference].astype(jnp.int32)


def draw_exch_kernel(key, part):
    spread = jnp.sqrt(jnp.float32(NOCC) / jnp.float32(NK * NAUX))
    base = jax.random.normal(jax.random.fold_in(key, 3), (NK, NAUX, NAUX), jnp.float32)
    symmetric = (base + jnp.transpose(base, (0, 2, 1))) * 0.7071
    return (symmetric * spread).astype(jnp.bfloat16)


def levels(stream_key, shape, split, smallest, high):
    factor_of = 1.0
    for position, blocks in split:
        draws = jax.random.uniform(jax.random.fold_in(jax.random.fold_in(stream_key, 6), position), (blocks,), jnp.float32, smallest / len(split), high / len(split))
        factor_of = factor_of * jnp.repeat(jnp.exp(draws), shape[position] // blocks).reshape((-1,) + (1,) * (len(shape) - 1 - position))
    return factor_of


def normal_values(key, shape, scale, reach, shards=(), held_as=jnp.bfloat16):
    result = scale * jax.random.normal(key, shape, jnp.float32)
    if shards:
        result = result * levels(key, shape, shards, -0.22, 0.18)
    return jnp.clip(result, -reach, reach).astype(held_as)


def setup_inputs(seed: int = 0) -> dict:
    key_list = jax.random.split(jax.random.key(seed), 9)
    occ_rows = normal_values(key_list[0], (NK, NAUX, NOCC), NOCC ** -0.5, 0.5, ((0, 8), (1, 4)))
    vir_rows = normal_values(key_list[1], (NK, NAUX, NVIR), NVIR ** -0.5, 0.1875, ((0, 8), (1, 4)))
    trial_vectors = normal_values(key_list[2], (NK, NVEC, NOCC, NVIR), 1.0, 6.0, ((0, 8), (3, 4)), jnp.float32)
    occ_energy = jnp.clip(-1.2 + 0.90000004 * jax.random.uniform(key_list[3], (NK, NOCC), jnp.float32) ** levels(key_list[3], (NK, NOCC), ((0, 8),), -0.2, 0.2), -1.2, -0.3)
    vir_energy = jnp.clip(0.1 + 1.4 * jax.random.uniform(key_list[4], (NK, NVIR), jnp.float32) ** levels(key_list[4], (NK, NVIR), ((0, 8), (1, 4)), -0.2, 0.2), 0.1, 1.5)
    coulomb = normal_values(key_list[5], (NAUX, NAUX), (NK * NAUX // 4) ** -0.5, 0.09375, ((0, 4),))
    exch_kernel = draw_exch_kernel(jax.random.fold_in(key_list[8], 71), 0)
    minus_table = draw_minus_table(jax.random.fold_in(key_list[8], 71), 0)
    return dict(occ_rows=occ_rows, vir_rows=vir_rows, trial_vectors=trial_vectors, occ_energy=occ_energy, vir_energy=vir_energy, coulomb=coulomb, exch_kernel=exch_kernel, minus_table=minus_table)


def reference(occ_rows, vir_rows, trial_vectors, occ_energy, vir_energy, coulomb, exch_kernel, minus_table):
    highest = lax.Precision.HIGHEST
    trial_half = trial_vectors.astype(jnp.bfloat16)

    def build_pairs(kpoint):
        occ_here = occ_rows[kpoint].astype(jnp.float32)
        vir_here = vir_rows[kpoint].astype(jnp.float32)
        mixed_rows = jnp.einsum("ri,via->vra", occ_here, trial_half[kpoint].astype(jnp.float32), precision=highest)
        mixed_rows = mixed_rows.astype(jnp.bfloat16)
        pair_block = jnp.einsum("vra,na->vrn", mixed_rows.astype(jnp.float32), vir_here, precision=highest)
        density_here = jnp.sum(mixed_rows.astype(jnp.float32) * vir_here[None], axis=2)
        return pair_block.astype(jnp.bfloat16), density_here

    pair_blocks, densities = lax.map(build_pairs, jnp.arange(NK, dtype=jnp.int32))
    density_half = jnp.sum(densities, axis=0).astype(jnp.bfloat16)
    potential = jnp.einsum("vn,rn->vr", density_half.astype(jnp.float32), coulomb.astype(jnp.float32), precision=highest)

    def build_sigma(kpoint):
        def add_transfer(running, momentum):
            source = minus_table[kpoint, momentum]
            weighted = pair_blocks[source].astype(jnp.float32) * exch_kernel[momentum].astype(jnp.float32)[None]
            return running + weighted, None

        screened, unused = lax.scan(add_transfer, jnp.zeros((NVEC, NAUX, NAUX), jnp.float32), jnp.arange(NK, dtype=jnp.int32))
        screened = screened.astype(jnp.bfloat16)
        vir_here = vir_rows[kpoint].astype(jnp.float32)
        product = jnp.einsum("vrn,na->vra", screened.astype(jnp.float32), vir_here, precision=highest)
        weights = (2.0 * potential[:, :, None] * vir_here[None] - product).astype(jnp.bfloat16)
        coupled = jnp.einsum("ri,vra->via", occ_rows[kpoint].astype(jnp.float32), weights.astype(jnp.float32), precision=highest)
        energy_gaps = vir_energy[kpoint][None, :] - occ_energy[kpoint][:, None]
        return energy_gaps[None] * trial_vectors[kpoint] + coupled

    return lax.map(build_sigma, jnp.arange(NK, dtype=jnp.int32))
```

```python
import functools

import jax
import jax.numpy as jnp
from jax import lax
from jax.experimental import pallas as pl
from jax.experimental.pallas import tpu as pltpu
from jax.sharding import PartitionSpec as P


def exchange_kernel(
    self_ref, table_ref, y_ref, occ_ref, exch_ref, z_ref, where_ref, wide_ref, pair_ref, scr_ref, acc_ref
):
    kpoints, points, width = y_ref.shape
    tile, nocc = occ_ref.shape[1], occ_ref.shape[2]
    vectors = width // nocc
    step = pl.program_id(0)

    @pl.when(step == 0)
    def _():
        for k in range(kpoints):
            for q in range(kpoints):
                where_ref[k, table_ref[k, q]] = q
        acc_ref[...] = jnp.zeros_like(acc_ref)

    for k in range(kpoints):
        wide_ref[k] = exch_ref[k].astype(jnp.float32)
        stacked = jnp.concatenate(
            [y_ref[k, :, v * nocc : (v + 1) * nocc] for v in range(vectors)], axis=0
        )
        pair_ref[k] = lax.dot_general(
            stacked, occ_ref[k], (((1,), (1,)), ((), ())), preferred_element_type=jnp.float32
        )
    rows, lanes = 16, 128
    for r in range(points // rows):
        @pl.loop(0, tile // lanes)
        def _(c):
            cols = pl.ds(pl.multiple_of(c * lanes, lanes), lanes)
            held = [
                [pair_ref[m, pl.ds(v * points + r * rows, rows), cols] for m in range(kpoints)]
                for v in range(vectors)
            ]
            for k in range(kpoints):
                total = [None] * vectors
                for m in range(kpoints):
                    kern = wide_ref[where_ref[k, m], pl.ds(r * rows, rows), cols]
                    for v in range(vectors):
                        term = held[v][m] * kern
                        total[v] = term if total[v] is None else total[v] + term
                for v in range(vectors):
                    scr_ref[k, pl.ds(v * points + r * rows, rows), cols] = total[v].astype(jnp.bfloat16)
    for k in range(kpoints):
        acc_ref[k] += jnp.dot(scr_ref[k], occ_ref[k], preferred_element_type=jnp.float32)

    @pl.when(step == pl.num_programs(0) - 1)
    def _():
        for k in range(kpoints):
            for v in range(vectors):
                z_ref[k, :, v * nocc : (v + 1) * nocc] = acc_ref[
                    k, v * points : (v + 1) * points, :
                ].astype(z_ref.dtype)


def exchange(self_point, table, y_all, occ_all, exch):
    kpoints, points, width = y_all.shape
    auxiliary, nocc = occ_all.shape[1], occ_all.shape[2]
    tile = min(256, auxiliary)
    stacked = points * width // nocc
    grid_spec = pltpu.PrefetchScalarGridSpec(
        num_scalar_prefetch=2,
        grid=(auxiliary // tile,),
        in_specs=[
            pl.BlockSpec((kpoints, points, width), lambda t, s, tab: (0, 0, 0)),
            pl.BlockSpec((kpoints, tile, nocc), lambda t, s, tab: (0, t, 0)),
            pl.BlockSpec((kpoints, points, tile), lambda t, s, tab: (0, s[0], t)),
        ],
        out_specs=pl.BlockSpec((kpoints, points, width), lambda t, s, tab: (0, 0, 0)),
        scratch_shapes=[
            pltpu.SMEM((kpoints, kpoints), jnp.int32),
            pltpu.VMEM((kpoints, points, tile), jnp.float32),
            pltpu.VMEM((kpoints, stacked, tile), jnp.float32),
            pltpu.VMEM((kpoints, stacked, tile), jnp.bfloat16),
            pltpu.VMEM((kpoints, stacked, nocc), jnp.float32),
        ],
    )
    flops = 4 * kpoints * stacked * auxiliary * nocc
    return pl.pallas_call(
        exchange_kernel,
        grid_spec=grid_spec,
        out_shape=jax.ShapeDtypeStruct((kpoints, points, width), jnp.bfloat16),
        compiler_params=pltpu.CompilerParams(dimension_semantics=("arbitrary",)),
        cost_estimate=pl.CostEstimate(
            flops=16 * flops,
            bytes_accessed=2 * kpoints * auxiliary * (nocc + points),
            transcendentals=0,
        ),
    )(self_point, table, y_all, occ_all, exch)


def per_device(
    occ_rows, vir_rows, trial_vectors, occ_energy, vir_energy, coulomb, exch_kernel, minus_table
):
    vectors, nocc, own_virtual = trial_vectors.shape[1:]
    own_rows = occ_rows.shape[1]
    kpoints = lax.axis_size("ka")
    bands = lax.axis_size("band")
    self_point = lax.axis_index("ka").astype(jnp.int32).reshape(1)
    occ_own, vir_own = occ_rows[0], vir_rows[0]
    points = own_rows // kpoints
    width = vectors * nocc

    trial_rows = jnp.transpose(trial_vectors[0].astype(jnp.bfloat16), (2, 0, 1))
    trial_full = lax.all_gather(
        trial_rows.reshape(own_virtual, width), "band", axis=0, tiled=True
    )
    occ_all = lax.all_gather(occ_own, ("ka", "band"), axis=0, tiled=True)
    occ_all = occ_all.reshape(kpoints, bands * own_rows, nocc)

    mapped = jnp.dot(vir_own, trial_full, preferred_element_type=jnp.float32)
    y_own = mapped.astype(jnp.bfloat16)
    y_all = lax.all_to_all(
        y_own.reshape(kpoints, points, width), "ka", split_axis=0, concat_axis=0, tiled=True
    )
    occ_wide = occ_own.astype(jnp.float32)
    density_own = jnp.sum(
        y_own.astype(jnp.float32).reshape(own_rows, vectors, nocc) * occ_wide[:, None, :], axis=2
    )
    density_sum = lax.psum(density_own.T, "ka")
    density_half = lax.all_gather(density_sum.astype(jnp.bfloat16), "band", axis=1, tiled=True)
    potential = jnp.einsum("vn,rn->rv", density_half, coulomb, preferred_element_type=jnp.float32)

    z_all = exchange(self_point, minus_table, y_all, occ_all, exch_kernel)
    z_own = lax.all_to_all(z_all, "ka", split_axis=0, concat_axis=0, tiled=True)
    z_own = z_own.reshape(own_rows, vectors, nocc)
    coupling = 2.0 * potential[:, :, None] * occ_wide[:, None, :] - z_own.astype(jnp.float32)
    coupling = coupling.astype(jnp.bfloat16).reshape(own_rows, width)
    partial_sums = lax.dot_general(
        vir_own, coupling, (((0,), (0,)), ((), ())), preferred_element_type=jnp.float32
    )
    parts = lax.all_to_all(
        partial_sums.astype(jnp.bfloat16).reshape(bands, own_virtual, width),
        "band",
        split_axis=0,
        concat_axis=0,
        tiled=True,
    )
    coupled = jnp.sum(parts.astype(jnp.float32), axis=0).reshape(own_virtual, vectors, nocc)
    coupled = jnp.transpose(coupled, (1, 2, 0))
    energy_gaps = vir_energy[0][None, :] - occ_energy[0][:, None]
    return (energy_gaps[None] * trial_vectors[0] + coupled)[None]


def solution(mesh):
    in_specs = (
        P("ka", "band", None),
        P("ka", "band", None),
        P("ka", None, None, "band"),
        P("ka", None),
        P("ka", "band"),
        P("band", None),
        P(None, "band", None),
        P(),
    )
    out_specs = P("ka", None, None, "band")
    return jax.shard_map(
        per_device, mesh=mesh, in_specs=in_specs, out_specs=out_specs, check_vma=False
    )
```

```python
import functools

import jax
import jax.numpy as jnp
from jax import lax
from jax.experimental import pallas as pl
from jax.experimental.pallas import tpu as pltpu
from jax.sharding import PartitionSpec as P


ROWS = 16
EXTRA = 16


def prepare_kernel(vir_ref, trial_ref, occ_ref, out_ref):
    kpoints, packed, width = out_ref.shape
    rows, nocc = occ_ref.shape
    points = rows // kpoints
    vectors = width // nocc
    mapped = jnp.dot(vir_ref[...], trial_ref[...], preferred_element_type=jnp.float32)
    mapped = mapped.astype(jnp.bfloat16)
    occ = occ_ref[...].astype(jnp.float32)
    ones = jnp.ones((EXTRA, nocc), jnp.bfloat16)
    place = lax.broadcasted_iota(jnp.int32, (EXTRA, width), 0)
    extra = jnp.zeros((EXTRA, width), jnp.float32)
    index = 0
    over_lanes = (((1,), (1,)), ((), ()))
    for v in range(vectors):
        terms = mapped[:, v * nocc : (v + 1) * nocc].astype(jnp.float32) * occ
        high = terms.astype(jnp.bfloat16)
        low = (terms - high.astype(jnp.float32)).astype(jnp.bfloat16)
        summed = lax.dot_general(ones, high, over_lanes, preferred_element_type=jnp.float32)
        summed += lax.dot_general(ones, low, over_lanes, preferred_element_type=jnp.float32)
        for start in range(0, rows, width):
            piece = summed[:, start : start + width]
            high_piece = piece.astype(jnp.bfloat16).astype(jnp.float32)
            extra = jnp.where(place == index, high_piece, extra)
            extra = jnp.where(place == index + EXTRA // 2, piece - high_piece, extra)
            index += 1
    extra = extra.astype(jnp.bfloat16)
    for j in range(kpoints):
        out_ref[j, :points] = mapped[j * points : (j + 1) * points]
        out_ref[j, points:] = extra


def prepare(kpoints, vir_own, trial_full, occ_own):
    rows = occ_own.shape[0]
    width = trial_full.shape[1]
    return pl.pallas_call(
        prepare_kernel,
        out_shape=jax.ShapeDtypeStruct((kpoints, rows // kpoints + EXTRA, width), jnp.bfloat16),
        cost_estimate=pl.CostEstimate(
            flops=2 * vir_own.size * width, bytes_accessed=2 * vir_own.size, transcendentals=0
        ),
    )(vir_own, trial_full, occ_own)


def exchange_kernel(with_total, first, place_ref, table_ref, *refs):
    if with_total:
        total_ref, refs = refs[0], refs[1:]
    y_ref, exch_hbm, refs = refs[0], refs[1], refs[2:]
    z_ref, where_ref, occ_ref, exch_ref, pair_ref, scr_ref, acc_ref, arrived = refs[-8:]
    blocks = refs[:-8]
    chunks, kpoints, points, rows = exch_ref.shape
    tile, nocc = pair_ref.shape[2], occ_ref.shape[4]
    tiles = rows // tile
    vectors = z_ref.shape[2] // nocc
    own = place_ref[0]

    copies = []
    for c in range(chunks):
        columns = pl.ds(pl.multiple_of(place_ref[1 + first + c] * rows, rows), rows)
        points_here = pl.ds(pl.multiple_of(own * points, points), points)
        copies.append(
            [
                pltpu.make_async_copy(blocks[2 * c], occ_ref.at[c, 0], arrived.at[c, 0]),
                pltpu.make_async_copy(blocks[2 * c + 1], occ_ref.at[c, 1], arrived.at[c, 1]),
                pltpu.make_async_copy(
                    exch_hbm.at[:, points_here, columns], exch_ref.at[c], arrived.at[c, 2]
                ),
            ]
        )
    for group in copies:
        for copy in group:
            copy.start()
    for k in range(kpoints):
        for q in range(kpoints):
            where_ref[k, q] = table_ref[own ^ k, q] ^ own
        for v in range(vectors):
            part = slice(v * points, (v + 1) * points)
            if with_total:
                acc_ref[k, part] = total_ref[own ^ k, :, v * nocc : (v + 1) * nocc]
            else:
                acc_ref[k, part] = jnp.zeros((points, nocc), jnp.float32)

    for c in range(chunks):
        for copy in copies[c]:
            copy.wait()

        @pl.loop(0, tiles)
        def _(t):
            here = pl.ds(pl.multiple_of(t * tile, tile), tile)
            for s in range(kpoints):
                y_here = y_ref[own ^ s]
                stacked = jnp.concatenate(
                    [y_here[:points, v * nocc : (v + 1) * nocc] for v in range(vectors)], axis=0
                )
                pair_ref[s] = lax.dot_general(
                    stacked,
                    occ_ref[c, s % 2, s // 2, here],
                    (((1,), (1,)), ((), ())),
                    preferred_element_type=jnp.float32,
                )
            for r in range(0, points, ROWS):
                kern = [
                    exch_ref[c, q, r : r + ROWS, here].astype(jnp.float32) for q in range(kpoints)
                ]
                for k in range(kpoints):
                    total = [None] * vectors
                    for q in range(kpoints):
                        source = where_ref[k, q]
                        for v in range(vectors):
                            at = v * points + r
                            term = pair_ref[source, at : at + ROWS] * kern[q]
                            total[v] = term if total[v] is None else total[v] + term
                    for v in range(vectors):
                        at = v * points + r
                        scr_ref[k, at : at + ROWS] = total[v].astype(jnp.bfloat16)
            for s in range(kpoints):
                acc_ref[s] += jnp.dot(
                    scr_ref[s],
                    occ_ref[c, s % 2, s // 2, here],
                    preferred_element_type=jnp.float32,
                )

    for s in range(kpoints):
        for v in range(vectors):
            z_ref[own ^ s, :, v * nocc : (v + 1) * nocc] = acc_ref[
                s, v * points : (v + 1) * points
            ].astype(z_ref.dtype)


def exchange(place, table, total, y_all, blocks, first, exch, out_type):
    kpoints, packed, width = y_all.shape
    half, rows, nocc = blocks[0].shape
    chunks = len(blocks) // 2
    points = rows // kpoints
    tile = min(256, rows)
    stacked = points * width // nocc
    totals = [] if total is None else [total]
    scalars = [pl.BlockSpec(memory_space=pltpu.SMEM)] * 2
    held = [pl.BlockSpec(memory_space=pltpu.VMEM)] * (len(totals) + 1)
    flops = 4 * kpoints * stacked * chunks * rows * nocc
    return pl.pallas_call(
        functools.partial(exchange_kernel, total is not None, first),
        in_specs=scalars + held + [pl.BlockSpec(memory_space=pl.ANY)] * (1 + len(blocks)),
        out_specs=pl.BlockSpec(memory_space=pltpu.VMEM),
        scratch_shapes=[
            pltpu.SMEM((kpoints, kpoints), jnp.int32),
            pltpu.VMEM((chunks, 2, half, rows, nocc), jnp.bfloat16),
            pltpu.VMEM((chunks, kpoints, points, rows), jnp.bfloat16),
            pltpu.VMEM((kpoints, stacked, tile), jnp.float32),
            pltpu.VMEM((kpoints, stacked, tile), jnp.bfloat16),
            pltpu.VMEM((kpoints, stacked, nocc), jnp.float32),
            pltpu.SemaphoreType.DMA((chunks, 3)),
        ],
        out_shape=jax.ShapeDtypeStruct((kpoints, points, width), out_type),
        cost_estimate=pl.CostEstimate(
            flops=16 * flops,
            bytes_accessed=2 * kpoints * chunks * rows * (nocc + points),
            transcendentals=0,
        ),
    )(place, table, *totals, y_all, exch, *blocks)


def potential_kernel(coulomb_ref, density_ref, occ_ref, out_ref):
    bands, vectors, rows = density_ref.shape
    nocc = occ_ref.shape[1]
    total = None
    for b in range(bands):
        density = density_ref[b].astype(jnp.float32)
        spread = jnp.concatenate(
            [jnp.broadcast_to(density[v : v + 1], (nocc, rows)) for v in range(vectors)], axis=0
        ).astype(jnp.bfloat16)
        term = lax.dot_general(
            coulomb_ref[:, b * rows : (b + 1) * rows],
            spread,
            (((1,), (1,)), ((), ())),
            preferred_element_type=jnp.float32,
        )
        total = term if total is None else total + term
    occ = 2.0 * occ_ref[...].astype(jnp.float32)
    for v in range(vectors):
        out_ref[:, v * nocc : (v + 1) * nocc] = total[:, v * nocc : (v + 1) * nocc] * occ


def hartree(coulomb, density, occ_own):
    rows, nocc = occ_own.shape
    width = density.shape[1] * nocc
    return pl.pallas_call(
        potential_kernel,
        out_shape=jax.ShapeDtypeStruct((rows, width), jnp.float32),
        cost_estimate=pl.CostEstimate(
            flops=2 * coulomb.size * width, bytes_accessed=2 * coulomb.size, transcendentals=0
        ),
    )(coulomb, density, occ_own)


def finish_kernel(direct_ref, z_ref, vir_ref, out_ref):
    coupling = (direct_ref[...] - z_ref[...].astype(jnp.float32)).astype(jnp.bfloat16)
    out_ref[...] = lax.dot_general(
        vir_ref[...], coupling, (((0,), (0,)), ((), ())), preferred_element_type=jnp.float32
    ).astype(jnp.bfloat16)


def finish(direct, z_own, vir_own):
    width = direct.shape[1]
    return pl.pallas_call(
        finish_kernel,
        out_shape=jax.ShapeDtypeStruct((vir_own.shape[1], width), jnp.bfloat16),
        cost_estimate=pl.CostEstimate(
            flops=2 * vir_own.size * width, bytes_accessed=2 * vir_own.size, transcendentals=0
        ),
    )(direct, z_own, vir_own)


def swap(x, axis, offset):
    return lax.ppermute(x, axis, [(i, i ^ offset) for i in range(lax.axis_size(axis))])


def over_chips(block):
    kpoints = lax.axis_size("ka")
    return jnp.stack([block] + [swap(block, "ka", s) for s in range(2, kpoints, 2)])


def gathered(block):
    bands = lax.axis_size("band")
    copies = jnp.broadcast_to(block[None], (bands,) + block.shape)
    return copies, lax.all_to_all(copies, "band", split_axis=0, concat_axis=0, tiled=True)


def per_device(
    occ_rows, vir_rows, trial_vectors, occ_energy, vir_energy, coulomb, exch_kernel, minus_table
):
    vectors, nocc, own_virtual = trial_vectors.shape[1:]
    own_rows = occ_rows.shape[1]
    kpoints = lax.axis_size("ka")
    bands = lax.axis_size("band")
    self_point = lax.axis_index("ka").astype(jnp.int32)
    self_band = lax.axis_index("band").astype(jnp.int32)
    occ_own, vir_own = occ_rows[0], vir_rows[0]
    points = own_rows // kpoints
    width = vectors * nocc
    lanes = jnp.arange(bands + 1, dtype=jnp.int32)
    place = jnp.where(lanes == 0, self_point, self_band ^ (lanes - 1))

    trial_rows = jnp.transpose(trial_vectors[0].astype(jnp.bfloat16), (2, 0, 1))
    copies, trial_full = gathered(trial_rows.reshape(own_virtual, width))
    trial_full = trial_full.reshape(bands * own_virtual, width)

    occ_sent, copies = lax.optimization_barrier((occ_own, copies))
    near = over_chips(occ_sent)
    blocks = []
    for s in range(bands):
        here = near if s == 0 else swap(near, "band", s)
        blocks += [here, swap(here, "ka", 1)]

    y_own = prepare(kpoints, vir_own, trial_full, occ_own)
    y_all = lax.all_to_all(y_own, "ka", split_axis=0, concat_axis=0, tiled=True)

    count = vectors * own_rows // width
    halves = jnp.sum(y_all[:, points:].astype(jnp.float32), axis=0)
    density_sum = halves[:count] + halves[EXTRA // 2 : EXTRA // 2 + count]
    density_sum = density_sum.reshape(vectors, own_rows)
    density_half = gathered(density_sum.astype(jnp.bfloat16))[1]
    direct = hartree(coulomb, density_half, occ_own)

    early = 2 * (bands - 1)
    z_all = exchange(
        place, minus_table, None, y_all, blocks[:early], 0, exch_kernel, jnp.float32
    )
    z_all = exchange(
        place, minus_table, z_all, y_all, blocks[early:], bands - 1, exch_kernel, jnp.bfloat16
    )

    z_own = lax.all_to_all(z_all, "ka", split_axis=0, concat_axis=0, tiled=True)
    partial_sums = finish(direct, z_own.reshape(own_rows, width), vir_own)
    parts = lax.all_to_all(
        partial_sums.reshape(bands, own_virtual, width),
        "band",
        split_axis=0,
        concat_axis=0,
        tiled=True,
    )
    coupled = jnp.sum(parts.astype(jnp.float32), axis=0).reshape(own_virtual, vectors, nocc)
    coupled = jnp.transpose(coupled, (1, 2, 0))
    energy_gaps = vir_energy[0][None, :] - occ_energy[0][:, None]
    return (energy_gaps[None] * trial_vectors[0] + coupled)[None]


def solution(mesh):
    in_specs = (
        P("ka", "band", None),
        P("ka", "band", None),
        P("ka", None, None, "band"),
        P("ka", None),
        P("ka", "band"),
        P("band", None),
        P(None, "band", None),
        P(),
    )
    out_specs = P("ka", None, None, "band")
    return jax.shard_map(
        per_device, mesh=mesh, in_specs=in_specs, out_specs=out_specs, check_vma=False
    )
```

```python
import jax
import jax.numpy as jnp
from jax import lax
from jax.experimental import pallas as pl
from jax.experimental.pallas import tpu as pltpu
from jax.sharding import PartitionSpec as P


MIB = 1024 * 1024
ROWS = 16
EXTRA = 16


def spread_kernel(trial_ref, out_ref):
    copies = out_ref.shape[0]
    vectors, _, nocc = trial_ref.shape
    for v in range(vectors):
        rounded = trial_ref[v].astype(jnp.bfloat16)
        for b in range(copies):
            out_ref[b, :, v * nocc : (v + 1) * nocc] = rounded


def spread(trial, copies):
    vectors, virtual, nocc = trial.shape
    return pl.pallas_call(
        spread_kernel,
        out_shape=jax.ShapeDtypeStruct((copies, virtual, vectors * nocc), jnp.bfloat16),
        compiler_params=pltpu.CompilerParams(vmem_limit_bytes=12 * MIB),
    )(trial)


def prepare_kernel(vir_ref, trial_ref, occ_hbm, out_ref, occ_ref, arrived):
    copy = pltpu.make_async_copy(occ_hbm, occ_ref, arrived)
    copy.start()
    kpoints, _, width = out_ref.shape
    rows, nocc = occ_ref.shape
    points = rows // kpoints
    vectors = width // nocc
    mapped = jnp.dot(vir_ref[...], trial_ref[...], preferred_element_type=jnp.float32)
    mapped = mapped.astype(jnp.bfloat16)
    copy.wait()
    occ = occ_ref[...].astype(jnp.float32)
    ones = jnp.ones((EXTRA, nocc), jnp.bfloat16)
    place = lax.broadcasted_iota(jnp.int32, (EXTRA, width), 0)
    extra = jnp.zeros((EXTRA, width), jnp.float32)
    index = 0
    over_lanes = (((1,), (1,)), ((), ()))
    for v in range(vectors):
        terms = mapped[:, v * nocc : (v + 1) * nocc].astype(jnp.float32) * occ
        high = terms.astype(jnp.bfloat16)
        low = (terms - high.astype(jnp.float32)).astype(jnp.bfloat16)
        summed = lax.dot_general(ones, high, over_lanes, preferred_element_type=jnp.float32)
        summed += lax.dot_general(ones, low, over_lanes, preferred_element_type=jnp.float32)
        for start in range(0, rows, width):
            piece = summed[:, start : start + width]
            high_piece = piece.astype(jnp.bfloat16).astype(jnp.float32)
            extra = jnp.where(place == index, high_piece, extra)
            extra = jnp.where(place == index + EXTRA // 2, piece - high_piece, extra)
            index += 1
    extra = extra.astype(jnp.bfloat16)
    for j in range(kpoints):
        out_ref[j, :points] = mapped[j * points : (j + 1) * points]
        out_ref[j, points:] = extra


def prepare(kpoints, vir_own, trial_full, occ_own):
    rows = occ_own.shape[0]
    width = trial_full.shape[1]
    return pl.pallas_call(
        prepare_kernel,
        in_specs=[pl.BlockSpec(memory_space=pltpu.VMEM)] * 2
        + [pl.BlockSpec(memory_space=pl.ANY)],
        out_specs=pl.BlockSpec(memory_space=pltpu.VMEM),
        scratch_shapes=[pltpu.VMEM(occ_own.shape, jnp.bfloat16), pltpu.SemaphoreType.DMA],
        out_shape=jax.ShapeDtypeStruct((kpoints, rows // kpoints + EXTRA, width), jnp.bfloat16),
        compiler_params=pltpu.CompilerParams(vmem_limit_bytes=12 * MIB),
        cost_estimate=pl.CostEstimate(
            flops=2 * vir_own.size * width, bytes_accessed=2 * vir_own.size, transcendentals=0
        ),
    )(vir_own, trial_full, occ_own)


def exchange_kernel(y_ref, table_hbm, exch_hbm, *refs):
    z_ref, table_ref, where_ref, occ_ref, exch_ref, pair_ref, scr_ref, acc_ref, arrived, known = refs[-10:]
    blocks = refs[:-10]
    count, kpoints, points, rows = exch_ref.shape
    tile, nocc = pair_ref.shape[2], occ_ref.shape[4]
    vectors = z_ref.shape[2] // nocc
    own = lax.axis_index("ka").astype(jnp.int32)
    band = lax.axis_index("band").astype(jnp.int32)

    table_copy = pltpu.make_async_copy(table_hbm, table_ref, known)
    table_copy.start()
    copies = []
    mine = pl.ds(pl.multiple_of(own * points, points), points)
    for c in range(count):
        first = pl.multiple_of((band ^ c) * rows, rows)
        copies.append(
            [
                pltpu.make_async_copy(blocks[2 * c], occ_ref.at[c, 0], arrived.at[c, 0]),
                pltpu.make_async_copy(blocks[2 * c + 1], occ_ref.at[c, 1], arrived.at[c, 1]),
                pltpu.make_async_copy(
                    exch_hbm.at[:, mine, pl.ds(first, rows)], exch_ref.at[c], arrived.at[c, 2]
                ),
            ]
        )
    for group in copies:
        for copy in group:
            copy.start()
    acc_ref[...] = jnp.zeros_like(acc_ref)
    table_copy.wait()
    for k in range(kpoints):
        for q in range(kpoints):
            where_ref[k, q] = table_ref[own ^ k, q] ^ own

    for c in range(count):
        for copy in copies[c]:
            copy.wait()

        @pl.loop(0, rows // tile)
        def _(t):
            here = pl.ds(pl.multiple_of(t * tile, tile), tile)
            for s in range(kpoints):
                y_here = y_ref[own ^ s]
                stacked = jnp.concatenate(
                    [y_here[:points, v * nocc : (v + 1) * nocc] for v in range(vectors)], axis=0
                )
                pair_ref[s] = lax.dot_general(
                    stacked,
                    occ_ref[c, s % 2, s // 2, here],
                    (((1,), (1,)), ((), ())),
                    preferred_element_type=jnp.float32,
                )
            for r in range(0, points, ROWS):
                kern = [
                    exch_ref[c, q, r : r + ROWS, here].astype(jnp.float32) for q in range(kpoints)
                ]
                for k in range(kpoints):
                    total = [None] * vectors
                    for q in range(kpoints):
                        source = where_ref[k, q]
                        for v in range(vectors):
                            at = v * points + r
                            term = pair_ref[source, at : at + ROWS] * kern[q]
                            total[v] = term if total[v] is None else total[v] + term
                    for v in range(vectors):
                        at = v * points + r
                        scr_ref[k, at : at + ROWS] = total[v].astype(jnp.bfloat16)
            for s in range(kpoints):
                acc_ref[s] += jnp.dot(
                    scr_ref[s],
                    occ_ref[c, s % 2, s // 2, here],
                    preferred_element_type=jnp.float32,
                )

    for s in range(kpoints):
        for v in range(vectors):
            z_ref[own ^ s, :, v * nocc : (v + 1) * nocc] = acc_ref[
                s, v * points : (v + 1) * points
            ].astype(z_ref.dtype)


def exchange(table, y_all, blocks, exch):
    kpoints, _, width = y_all.shape
    half, rows, nocc = blocks[0].shape
    chunks = len(blocks) // 2
    points = rows // kpoints
    tile = min(256, rows)
    stacked = points * width // nocc
    held = pl.BlockSpec(memory_space=pltpu.VMEM)
    flops = 4 * kpoints * stacked * chunks * rows * nocc
    return pl.pallas_call(
        exchange_kernel,
        in_specs=[held] + [pl.BlockSpec(memory_space=pl.ANY)] * (2 + len(blocks)),
        out_specs=held,
        scratch_shapes=[
            pltpu.SMEM((kpoints, kpoints), jnp.int32),
            pltpu.SMEM((kpoints, kpoints), jnp.int32),
            pltpu.VMEM((chunks, 2, half, rows, nocc), jnp.bfloat16),
            pltpu.VMEM((chunks, kpoints, points, rows), jnp.bfloat16),
            pltpu.VMEM((kpoints, stacked, tile), jnp.float32),
            pltpu.VMEM((kpoints, stacked, tile), jnp.bfloat16),
            pltpu.VMEM((kpoints, stacked, nocc), jnp.float32),
            pltpu.SemaphoreType.DMA((chunks, 3)),
            pltpu.SemaphoreType.DMA,
        ],
        out_shape=jax.ShapeDtypeStruct((kpoints, points, width), jnp.bfloat16),
        cost_estimate=pl.CostEstimate(
            flops=16 * flops,
            bytes_accessed=2 * kpoints * chunks * rows * (nocc + points),
            transcendentals=0,
        ),
    )(y_all, table, exch, *blocks)


def density_kernel(y_ref, out_ref):
    vectors, rows = out_ref.shape
    width = y_ref.shape[2]
    pieces = rows // width
    points = y_ref.shape[1] - EXTRA
    halves = jnp.sum(y_ref[:, points:].astype(jnp.float32), axis=0)
    halves = halves[: EXTRA // 2] + halves[EXTRA // 2 :]
    out_ref[...] = jnp.concatenate(
        [
            jnp.concatenate(
                [halves[v * pieces + h : v * pieces + h + 1] for h in range(pieces)], axis=1
            )
            for v in range(vectors)
        ],
        axis=0,
    ).astype(jnp.bfloat16)


def summed_density(vectors, rows, y_all):
    return pl.pallas_call(
        density_kernel,
        out_shape=jax.ShapeDtypeStruct((vectors, rows), jnp.bfloat16),
        compiler_params=pltpu.CompilerParams(vmem_limit_bytes=4 * MIB),
    )(y_all)


def potential_kernel(coulomb_ref, occ_ref, *refs):
    density_refs, out_ref = refs[:-1], refs[-1]
    vectors, rows = density_refs[0].shape
    nocc = occ_ref.shape[1]
    band = lax.axis_index("band").astype(jnp.int32)
    total = None
    for b, density_ref in enumerate(density_refs):
        density = density_ref[...].astype(jnp.float32)
        first = pl.multiple_of((band ^ b) * rows, rows)
        spread = jnp.concatenate(
            [jnp.broadcast_to(density[v : v + 1], (nocc, rows)) for v in range(vectors)], axis=0
        ).astype(jnp.bfloat16)
        term = lax.dot_general(
            coulomb_ref[:, pl.ds(first, rows)],
            spread,
            (((1,), (1,)), ((), ())),
            preferred_element_type=jnp.float32,
        )
        total = term if total is None else total + term
    occ = 2.0 * occ_ref[...].astype(jnp.float32)
    for v in range(vectors):
        out_ref[:, v * nocc : (v + 1) * nocc] = total[:, v * nocc : (v + 1) * nocc] * occ


def hartree(coulomb, occ_own, densities):
    rows, nocc = occ_own.shape
    width = densities[0].shape[0] * nocc
    return pl.pallas_call(
        potential_kernel,
        out_shape=jax.ShapeDtypeStruct((rows, width), jnp.float32),
        compiler_params=pltpu.CompilerParams(vmem_limit_bytes=12 * MIB),
        cost_estimate=pl.CostEstimate(
            flops=2 * coulomb.size * width, bytes_accessed=2 * coulomb.size, transcendentals=0
        ),
    )(coulomb, occ_own, *densities)


def finish_kernel(direct_ref, z_ref, vir_ref, out_ref):
    coupling = (direct_ref[...] - z_ref[...].astype(jnp.float32)).astype(jnp.bfloat16)
    out_ref[...] = lax.dot_general(
        vir_ref[...], coupling, (((0,), (0,)), ((), ())), preferred_element_type=jnp.float32
    ).astype(jnp.bfloat16)


def finish(direct, z_own, vir_own):
    width = direct.shape[1]
    return pl.pallas_call(
        finish_kernel,
        out_shape=jax.ShapeDtypeStruct((vir_own.shape[1], width), jnp.bfloat16),
        compiler_params=pltpu.CompilerParams(vmem_limit_bytes=12 * MIB),
        cost_estimate=pl.CostEstimate(
            flops=2 * vir_own.size * width, bytes_accessed=2 * vir_own.size, transcendentals=0
        ),
    )(direct, z_own, vir_own)


def swap(x, axis, offset):
    return lax.ppermute(x, axis, [(i, i ^ offset) for i in range(lax.axis_size(axis))])


def over_chips(block):
    kpoints = lax.axis_size("ka")
    return [block] + [swap(block, "ka", s) for s in range(2, kpoints, 2)]


def trade(x, axis):
    return lax.all_to_all(x, axis, split_axis=0, concat_axis=0, tiled=True)


def per_device(
    occ_rows, vir_rows, trial_vectors, occ_energy, vir_energy, coulomb, exch_kernel, minus_table
):
    vectors, nocc, own_virtual = trial_vectors.shape[1:]
    own_rows = occ_rows.shape[1]
    kpoints = lax.axis_size("ka")
    bands = lax.axis_size("band")
    occ_own, vir_own = occ_rows[0], vir_rows[0]
    width = vectors * nocc
    copies = spread(jnp.swapaxes(trial_vectors[0], 1, 2), bands)
    trial_full = trade(copies, "band")
    trial_full = trial_full.reshape(bands * own_virtual, width)

    direct = [s for s in range(1, bands) if s & (s - 1) == 0]
    remote = [s for s in range(1, bands) if s & (s - 1)]
    parts = over_chips(occ_own)
    moved = {s: swap(occ_own, "band", s) for s in remote}

    y_own = prepare(kpoints, vir_own, trial_full, occ_own)
    y_all = trade(y_own, "ka")

    parts, y_own = lax.optimization_barrier((parts, y_own))
    near = {0: jnp.stack(parts)}
    near.update({s: swap(near[0], "band", s) for s in direct})
    near.update({s: jnp.stack(over_chips(moved[s])) for s in remote})

    density = summed_density(vectors, own_rows, y_all)
    densities = [density] + [swap(density, "band", s) for s in range(1, bands)]
    potential = hartree(coulomb, occ_own, densities)

    blocks = []
    for s in range(bands):
        blocks += [near[s], swap(near[s], "ka", 1)]
    z_all = exchange(minus_table, y_all, blocks, exch_kernel)

    z_own = trade(z_all, "ka")
    partial_sums = finish(potential, z_own.reshape(own_rows, width), vir_own)
    parts = trade(partial_sums.reshape(bands, own_virtual, width), "band")
    coupled = jnp.sum(parts.astype(jnp.float32), axis=0).reshape(own_virtual, vectors, nocc)
    coupled = jnp.transpose(coupled, (1, 2, 0))
    energy_gaps = vir_energy[0][None, :] - occ_energy[0][:, None]
    return (energy_gaps[None] * trial_vectors[0] + coupled)[None]


def solution(mesh):
    in_specs = (
        P("ka", "band", None),
        P("ka", "band", None),
        P("ka", None, None, "band"),
        P("ka", None),
        P("ka", "band"),
        P("band", None),
        P(None, "band", None),
        P(),
    )
    out_specs = P("ka", None, None, "band")

    return jax.shard_map(
        per_device, mesh=mesh, in_specs=in_specs, out_specs=out_specs, check_vma=False
    )
```

```python
import jax
import jax.numpy as jnp
from jax import lax
from jax.experimental import pallas as pl
from jax.experimental.pallas import tpu as pltpu
from jax.sharding import PartitionSpec as P


MIB = 1024 * 1024
ROWS = 16
EXTRA = 16


def round_kernel(trial_ref, out_ref):
    vectors, _, nocc = trial_ref.shape
    for v in range(vectors):
        out_ref[:, v * nocc : (v + 1) * nocc] = trial_ref[v].astype(jnp.bfloat16)


def rounded(trial):
    vectors, virtual, nocc = trial.shape
    return pl.pallas_call(
        round_kernel,
        out_shape=jax.ShapeDtypeStruct((virtual, vectors * nocc), jnp.bfloat16),
        compiler_params=pltpu.CompilerParams(vmem_limit_bytes=12 * MIB),
    )(trial)


def prepare_kernel(vir_ref, occ_hbm, *refs):
    parts, (out_ref, trial_ref, occ_ref, arrived) = refs[:-4], refs[-4:]
    copy = pltpu.make_async_copy(occ_hbm, occ_ref, arrived)
    copy.start()
    band = lax.axis_index("band").astype(jnp.int32)
    virtual = parts[0].shape[0]
    for s, part in enumerate(parts):
        trial_ref[pl.ds(pl.multiple_of((band ^ s) * virtual, 16), virtual)] = part[...]
    kpoints, _, width = out_ref.shape
    rows, nocc = occ_ref.shape
    points = rows // kpoints
    vectors = width // nocc
    mapped = jnp.dot(vir_ref[...], trial_ref[...], preferred_element_type=jnp.float32)
    mapped = mapped.astype(jnp.bfloat16)
    copy.wait()
    occ = occ_ref[...].astype(jnp.float32)
    ones = jnp.ones((EXTRA, nocc), jnp.bfloat16)
    place = lax.broadcasted_iota(jnp.int32, (EXTRA, width), 0)
    extra = jnp.zeros((EXTRA, width), jnp.float32)
    index = 0
    over_lanes = (((1,), (1,)), ((), ()))
    for v in range(vectors):
        terms = mapped[:, v * nocc : (v + 1) * nocc].astype(jnp.float32) * occ
        high = terms.astype(jnp.bfloat16)
        low = (terms - high.astype(jnp.float32)).astype(jnp.bfloat16)
        summed = lax.dot_general(ones, high, over_lanes, preferred_element_type=jnp.float32)
        summed += lax.dot_general(ones, low, over_lanes, preferred_element_type=jnp.float32)
        for start in range(0, rows, width):
            piece = summed[:, start : start + width]
            high_piece = piece.astype(jnp.bfloat16).astype(jnp.float32)
            extra = jnp.where(place == index, high_piece, extra)
            extra = jnp.where(place == index + EXTRA // 2, piece - high_piece, extra)
            index += 1
    extra = extra.astype(jnp.bfloat16)
    for j in range(kpoints):
        out_ref[j, :points] = mapped[j * points : (j + 1) * points]
        out_ref[j, points:] = extra


def prepare(kpoints, vir_own, parts, occ_own):
    rows = occ_own.shape[0]
    width = parts[0].shape[1]
    held = pl.BlockSpec(memory_space=pltpu.VMEM)
    return pl.pallas_call(
        prepare_kernel,
        in_specs=[held, pl.BlockSpec(memory_space=pl.ANY)] + [held] * len(parts),
        out_specs=held,
        scratch_shapes=[
            pltpu.VMEM((vir_own.shape[1], width), jnp.bfloat16),
            pltpu.VMEM(occ_own.shape, jnp.bfloat16),
            pltpu.SemaphoreType.DMA,
        ],
        out_shape=jax.ShapeDtypeStruct((kpoints, rows // kpoints + EXTRA, width), jnp.bfloat16),
        compiler_params=pltpu.CompilerParams(vmem_limit_bytes=12 * MIB),
        cost_estimate=pl.CostEstimate(
            flops=2 * vir_own.size * width, bytes_accessed=2 * vir_own.size, transcendentals=0
        ),
    )(vir_own, occ_own, *parts)


def exchange_kernel(y_ref, table_hbm, exch_hbm, *refs):
    z_ref, table_ref, where_ref, occ_ref, exch_ref, pair_ref, scr_ref, acc_ref, arrived, known = refs[-10:]
    blocks = refs[:-10]
    count, kpoints, points, rows = exch_ref.shape
    tile, nocc = pair_ref.shape[2], occ_ref.shape[4]
    vectors = z_ref.shape[2] // nocc
    own = lax.axis_index("ka").astype(jnp.int32)
    band = lax.axis_index("band").astype(jnp.int32)

    table_copy = pltpu.make_async_copy(table_hbm, table_ref, known)
    table_copy.start()
    copies = []
    mine = pl.ds(pl.multiple_of(own * points, points), points)
    for c in range(count):
        first = pl.multiple_of((band ^ c) * rows, rows)
        copies.append(
            [
                pltpu.make_async_copy(blocks[2 * c], occ_ref.at[c, 0], arrived.at[c, 0]),
                pltpu.make_async_copy(blocks[2 * c + 1], occ_ref.at[c, 1], arrived.at[c, 1]),
                pltpu.make_async_copy(
                    exch_hbm.at[:, mine, pl.ds(first, rows)], exch_ref.at[c], arrived.at[c, 2]
                ),
            ]
        )
    for group in copies:
        for copy in group:
            copy.start()
    acc_ref[...] = jnp.zeros_like(acc_ref)
    table_copy.wait()
    for k in range(kpoints):
        for q in range(kpoints):
            where_ref[k, q] = table_ref[own ^ k, q] ^ own

    for c in range(count):
        for copy in copies[c]:
            copy.wait()

        @pl.loop(0, rows // tile)
        def _(t):
            here = pl.ds(pl.multiple_of(t * tile, tile), tile)
            for s in range(kpoints):
                y_here = y_ref[own ^ s]
                stacked = jnp.concatenate(
                    [y_here[:points, v * nocc : (v + 1) * nocc] for v in range(vectors)], axis=0
                )
                pair_ref[s] = lax.dot_general(
                    stacked,
                    occ_ref[c, s % 2, s // 2, here],
                    (((1,), (1,)), ((), ())),
                    preferred_element_type=jnp.float32,
                )
            for r in range(0, points, ROWS):
                kern = [
                    exch_ref[c, q, r : r + ROWS, here].astype(jnp.float32) for q in range(kpoints)
                ]
                for k in range(kpoints):
                    total = [None] * vectors
                    for q in range(kpoints):
                        source = where_ref[k, q]
                        for v in range(vectors):
                            at = v * points + r
                            term = pair_ref[source, at : at + ROWS] * kern[q]
                            total[v] = term if total[v] is None else total[v] + term
                    for v in range(vectors):
                        at = v * points + r
                        scr_ref[k, at : at + ROWS] = total[v].astype(jnp.bfloat16)
            for s in range(kpoints):
                acc_ref[s] += jnp.dot(
                    scr_ref[s],
                    occ_ref[c, s % 2, s // 2, here],
                    preferred_element_type=jnp.float32,
                )

    for s in range(kpoints):
        for v in range(vectors):
            z_ref[own ^ s, :, v * nocc : (v + 1) * nocc] = acc_ref[
                s, v * points : (v + 1) * points
            ].astype(z_ref.dtype)


def exchange(table, y_all, blocks, exch):
    kpoints, _, width = y_all.shape
    half, rows, nocc = blocks[0].shape
    chunks = len(blocks) // 2
    points = rows // kpoints
    tile = min(256, rows)
    stacked = points * width // nocc
    held = pl.BlockSpec(memory_space=pltpu.VMEM)
    flops = 4 * kpoints * stacked * chunks * rows * nocc
    return pl.pallas_call(
        exchange_kernel,
        in_specs=[held] + [pl.BlockSpec(memory_space=pl.ANY)] * (2 + len(blocks)),
        out_specs=held,
        scratch_shapes=[
            pltpu.SMEM((kpoints, kpoints), jnp.int32),
            pltpu.SMEM((kpoints, kpoints), jnp.int32),
            pltpu.VMEM((chunks, 2, half, rows, nocc), jnp.bfloat16),
            pltpu.VMEM((chunks, kpoints, points, rows), jnp.bfloat16),
            pltpu.VMEM((kpoints, stacked, tile), jnp.float32),
            pltpu.VMEM((kpoints, stacked, tile), jnp.bfloat16),
            pltpu.VMEM((kpoints, stacked, nocc), jnp.float32),
            pltpu.SemaphoreType.DMA((chunks, 3)),
            pltpu.SemaphoreType.DMA,
        ],
        out_shape=jax.ShapeDtypeStruct((kpoints, points, width), jnp.bfloat16),
        cost_estimate=pl.CostEstimate(
            flops=16 * flops,
            bytes_accessed=2 * kpoints * chunks * rows * (nocc + points),
            transcendentals=0,
        ),
    )(y_all, table, exch, *blocks)


def density_kernel(y_ref, out_ref):
    vectors, rows = out_ref.shape
    width = y_ref.shape[2]
    pieces = rows // width
    points = y_ref.shape[1] - EXTRA
    halves = jnp.sum(y_ref[:, points:].astype(jnp.float32), axis=0)
    halves = halves[: EXTRA // 2] + halves[EXTRA // 2 :]
    out_ref[...] = jnp.concatenate(
        [
            jnp.concatenate(
                [halves[v * pieces + h : v * pieces + h + 1] for h in range(pieces)], axis=1
            )
            for v in range(vectors)
        ],
        axis=0,
    ).astype(jnp.bfloat16)


def summed_density(vectors, rows, y_all):
    return pl.pallas_call(
        density_kernel,
        out_shape=jax.ShapeDtypeStruct((vectors, rows), jnp.bfloat16),
        compiler_params=pltpu.CompilerParams(vmem_limit_bytes=4 * MIB),
    )(y_all)


def potential_kernel(coulomb_ref, occ_ref, *refs):
    density_refs, out_ref = refs[:-1], refs[-1]
    vectors, rows = density_refs[0].shape
    nocc = occ_ref.shape[1]
    band = lax.axis_index("band").astype(jnp.int32)
    total = None
    for b, density_ref in enumerate(density_refs):
        density = density_ref[...].astype(jnp.float32)
        first = pl.multiple_of((band ^ b) * rows, rows)
        spread = jnp.concatenate(
            [jnp.broadcast_to(density[v : v + 1], (nocc, rows)) for v in range(vectors)], axis=0
        ).astype(jnp.bfloat16)
        term = lax.dot_general(
            coulomb_ref[:, pl.ds(first, rows)],
            spread,
            (((1,), (1,)), ((), ())),
            preferred_element_type=jnp.float32,
        )
        total = term if total is None else total + term
    occ = 2.0 * occ_ref[...].astype(jnp.float32)
    for v in range(vectors):
        out_ref[:, v * nocc : (v + 1) * nocc] = total[:, v * nocc : (v + 1) * nocc] * occ


def hartree(coulomb, occ_own, densities):
    rows, nocc = occ_own.shape
    width = densities[0].shape[0] * nocc
    return pl.pallas_call(
        potential_kernel,
        out_shape=jax.ShapeDtypeStruct((rows, width), jnp.float32),
        compiler_params=pltpu.CompilerParams(vmem_limit_bytes=12 * MIB),
        cost_estimate=pl.CostEstimate(
            flops=2 * coulomb.size * width, bytes_accessed=2 * coulomb.size, transcendentals=0
        ),
    )(coulomb, occ_own, *densities)


def finish_kernel(direct_ref, z_ref, vir_ref, *refs):
    own_ref, sent_refs, total_ref = refs[0], refs[1:-1], refs[-1]
    rows = own_ref.shape[0]
    band = lax.axis_index("band").astype(jnp.int32)
    coupling = (direct_ref[...] - z_ref[...].astype(jnp.float32)).astype(jnp.bfloat16)
    total_ref[...] = lax.dot_general(
        vir_ref[...], coupling, (((0,), (0,)), ((), ())), preferred_element_type=jnp.float32
    )
    own_ref[...] = total_ref[pl.ds(pl.multiple_of(band * rows, 8), rows)]
    for s, sent_ref in enumerate(sent_refs):
        first = pl.multiple_of((band ^ (s + 1)) * rows, 8)
        sent_ref[...] = total_ref[pl.ds(first, rows)].astype(jnp.bfloat16)


def finish(direct, z_own, vir_own, bands):
    width = direct.shape[1]
    virtual = vir_own.shape[1]
    part = (virtual // bands, width)
    return pl.pallas_call(
        finish_kernel,
        out_shape=[jax.ShapeDtypeStruct(part, jnp.float32)]
        + [jax.ShapeDtypeStruct(part, jnp.bfloat16)] * (bands - 1),
        scratch_shapes=[pltpu.VMEM((virtual, width), jnp.float32)],
        compiler_params=pltpu.CompilerParams(vmem_limit_bytes=12 * MIB),
        cost_estimate=pl.CostEstimate(
            flops=2 * vir_own.size * width, bytes_accessed=2 * vir_own.size, transcendentals=0
        ),
    )(direct, z_own, vir_own)


def total_kernel(gap_ref, trial_ref, own_ref, *refs):
    received, out_ref = refs[:-1], refs[-1]
    vectors, _, nocc = out_ref.shape
    for v in range(vectors):
        part = slice(v * nocc, (v + 1) * nocc)
        coupled = own_ref[:, part]
        for ref in received:
            coupled += ref[:, part].astype(jnp.float32)
        out_ref[v] = gap_ref[...] * trial_ref[v] + coupled


def total(gaps, trial, own, received):
    return pl.pallas_call(
        total_kernel,
        out_shape=jax.ShapeDtypeStruct(trial.shape, jnp.float32),
        compiler_params=pltpu.CompilerParams(vmem_limit_bytes=12 * MIB),
    )(gaps, trial, own, *received)


def swap(x, axis, offset):
    return lax.ppermute(x, axis, [(i, i ^ offset) for i in range(lax.axis_size(axis))])


def over_chips(block):
    kpoints = lax.axis_size("ka")
    return [block] + [swap(block, "ka", s) for s in range(2, kpoints, 2)]


def trade(x, axis):
    return lax.all_to_all(x, axis, split_axis=0, concat_axis=0, tiled=True)


def per_device(
    occ_rows, vir_rows, trial_vectors, occ_energy, vir_energy, coulomb, exch_kernel, minus_table
):
    vectors, nocc, _ = trial_vectors.shape[1:]
    own_rows = occ_rows.shape[1]
    kpoints = lax.axis_size("ka")
    bands = lax.axis_size("band")
    occ_own, vir_own = occ_rows[0], vir_rows[0]
    width = vectors * nocc
    trial_own = rounded(jnp.swapaxes(trial_vectors[0], 1, 2))
    trials = [trial_own] + [swap(trial_own, "band", s) for s in range(1, bands)]

    direct = [s for s in range(1, bands) if s & (s - 1) == 0]
    remote = [s for s in range(1, bands) if s & (s - 1)]
    parts = over_chips(occ_own)
    moved = {s: swap(occ_own, "band", s) for s in remote}

    y_own = prepare(kpoints, vir_own, trials, occ_own)
    y_all = trade(y_own, "ka")

    parts, y_own = lax.optimization_barrier((parts, y_own))
    near = {0: jnp.stack(parts)}
    near.update({s: swap(near[0], "band", s) for s in direct})
    near.update({s: jnp.stack(over_chips(moved[s])) for s in remote})

    density = summed_density(vectors, own_rows, y_all)
    densities = [density] + [swap(density, "band", s) for s in range(1, bands)]
    potential = hartree(coulomb, occ_own, densities)

    blocks = []
    for s in range(bands):
        blocks += [near[s], swap(near[s], "ka", 1)]
    z_all = exchange(minus_table, y_all, blocks, exch_kernel)

    z_own = trade(z_all, "ka")
    own, *sent = finish(potential, z_own.reshape(own_rows, width), vir_own, bands)
    received = [swap(part, "band", s + 1) for s, part in enumerate(sent)]
    gaps = vir_energy[0][:, None] - occ_energy[0][None, :]
    sigma = total(gaps, jnp.swapaxes(trial_vectors[0], 1, 2), own, received)
    return jnp.swapaxes(sigma, 1, 2)[None]


def solution(mesh):
    in_specs = (
        P("ka", "band", None),
        P("ka", "band", None),
        P("ka", None, None, "band"),
        P("ka", None),
        P("ka", "band"),
        P("band", None),
        P(None, "band", None),
        P(),
    )
    out_specs = P("ka", None, None, "band")

    return jax.shard_map(
        per_device, mesh=mesh, in_specs=in_specs, out_specs=out_specs, check_vma=False
    )
```
